128 devices in a mesh: dp: 16 (over y_hi, z, core), tensor: 8 (over y_lo, x).
Axes of the slice: x: 4, y: 4 (y_hi: 2, y_lo: 2; y = y_hi * 2 + y_lo), z: 4, core: 2. Of those that a mesh axis runs over, the one named last changes fastest.
Arguments:
- saved_queries: bfloat16 [16384, 8192], P('dp', 'tensor'), may hold values from -200 to 200
- saved_keys: bfloat16 [16384, 1024], P('dp', 'tensor'), may hold values from -200 to 200
- saved_values: bfloat16 [16384, 1024], P('dp', 'tensor'), may hold values from -6 to 6
- out_grad: bfloat16 [16384, 8192], P(('dp', 'tensor')), may hold values from -2.5 to 2.5
- act_exponent: int32 [1], replicated, may hold values from -6 to 3
- grad_exponent: int32 [1], replicated, may hold values from -4 to 1
Outputs:
- grad_weight: float32 [8192, 8192], P('dp', 'tensor')
The draws below stay inside these ranges and needn't reach their ends.
All inputs are finite; a program needn't handle non-finite values.
Results may differ from the reference program's by a relative error of at most 0.012.
Values may be sent and summed in bfloat16 or wider, within the bound.
No kernel may reach another device: no remote copies, remote signals or barrier semaphores. Data moves between devices by JAX's collectives and lax.ppermute only.
A program may use at most 128 MiB of HBM per device.

```python
import jax
import jax.numpy as jnp
from jax import lax

D = 8192
HEADS = 64
KV_HEADS = 8
HEAD_DIM = 128
SEQ = 1024
TOKENS = 16384
N_DP = 16


def query_keys(key):
    base = jax.random.fold_in(key, 11)
    first, second = jax.random.split(base)
    queries = jnp.clip(jax.random.normal(first, (TOKENS, HEADS * HEAD_DIM), jnp.float32), -5.0, 5.0)
    keys_all = jnp.clip(jax.random.normal(second, (TOKENS, KV_HEADS * HEAD_DIM), jnp.float32), -5.0, 5.0)
    return (queries, keys_all)


def draw_saved_queries(key, part):
    return query_keys(key)[0].astype(jnp.bfloat16)


def draw_saved_keys(key, part):
    return query_keys(key)[1].astype(jnp.bfloat16)


def raised(entries, stream_key, source, target, parts, factor):
    def block_of(axis_at):
        return (jnp.arange(entries.shape[axis_at]) // (entries.shape[axis_at] // parts)).reshape((-1,) + (1,) * (entries.ndim - 1 - axis_at))

    near = jax.random.permutation(stream_key, parts)[block_of(target)]
    second = (block_of(target) + parts // 2) % parts
    return jnp.where((block_of(source) == near) | (block_of(source) == second), factor * entries, entries)


def steps_of(rng, extent, cuts, low, largest):
    factor_of = 1.0
    for dim, blocks in cuts:
        steps = jax.random.uniform(jax.random.fold_in(jax.random.fold_in(rng, 6), dim), (blocks,), jnp.float32, low / len(cuts), largest / len(cuts))
        factor_of = factor_of * jnp.repeat(jnp.exp(steps), extent[dim] // blocks).reshape((-1,) + (1,) * (len(extent) - 1 - dim))
    return factor_of


def centred(key, shape, deviation, reach, cuts=(), kind=jnp.bfloat16):
    array = jax.random.normal(key, shape, jnp.float32) * deviation
    if len(cuts) > 0:
        array = steps_of(key, shape, cuts, -0.22, 0.18) * array
    return jnp.clip(array, min=-reach, max=reach).astype(kind)


def heavy_noise(rng, shape, width, limit, shards, heavy, kind=jnp.bfloat16):
    drawn = width * jax.random.normal(rng, shape, jnp.float32)
    if shards:
        drawn = drawn * steps_of(rng, shape, shards, -0.22, 0.18)
    return jnp.clip(raised(drawn, jax.random.fold_in(rng, 3), *heavy), -limit, limit).astype(kind)


def setup_inputs(seed: int = 0) -> dict:
    splits = jax.random.split(jax.random.key(seed), 7)
    return {
        "saved_queries": draw_saved_queries(jax.random.fold_in(splits[6], 71), 0),
        "saved_keys": draw_saved_keys(jax.random.fold_in(splits[6], 71), 0),
        "saved_values": centred(splits[2], (TOKENS, KV_HEADS * HEAD_DIM), 1.0, 6.0, ((0, 16), (1, 8))),
        "out_grad": heavy_noise(splits[3], (TOKENS, D), 0.1, 2.5, ((0, 128),), (0, 1, 128, 5.5)),
        "act_exponent": jax.random.randint(splits[4], (1,), -6, 4).astype(jnp.int32),
        "grad_exponent": jax.random.randint(splits[5], (1,), -4, 2).astype(jnp.int32),
    }


SATURATION = 448.0

def quantize(values_in, exponent):
    factor = SATURATION * jnp.exp2(-exponent[0].astype(jnp.float32))
    return jnp.clip(values_in * factor, -SATURATION, SATURATION).astype(jnp.bfloat16)

def attend(query_rows, key_rows, value_rows):
    scores = jnp.dot(query_rows, key_rows.T, preferred_element_type=jnp.float32) * HEAD_DIM ** (-0.5)
    positions = jnp.arange(query_rows.shape[0], dtype=jnp.int32)
    causal = positions[None, :] <= positions[:, None]
    scores = jnp.where(causal, scores, jnp.float32(-1e+30))
    row_max = lax.optimization_barrier(jnp.max(scores, axis=1, keepdims=True))
    weights = jnp.exp(scores - row_max)
    probabilities = (weights / lax.optimization_barrier(jnp.sum(weights, axis=1, keepdims=True))).astype(jnp.bfloat16)
    return jnp.dot(probabilities, value_rows, preferred_element_type=jnp.float32)

def reference(saved_queries, saved_keys, saved_values, out_grad, act_exponent, grad_exponent):
    per_group = HEADS // KV_HEADS
    dequant = jnp.exp2((act_exponent[0] + grad_exponent[0]).astype(jnp.float32)) / (SATURATION * SATURATION)

    def sequence_grad(running, seq_index):
        offset = (seq_index * SEQ).astype(jnp.int32)
        seq_queries = lax.dynamic_slice_in_dim(saved_queries, offset, SEQ, 0)
        seq_keys = lax.dynamic_slice_in_dim(saved_keys, offset, SEQ, 0)
        seq_values = lax.dynamic_slice_in_dim(saved_values, offset, SEQ, 0)
        seq_grad = lax.dynamic_slice_in_dim(out_grad, offset, SEQ, 0)

        def one_head(head_index):
            query_rows = lax.dynamic_slice_in_dim(seq_queries, (head_index * HEAD_DIM).astype(jnp.int32), HEAD_DIM, 1)
            kv_start = (head_index // per_group * HEAD_DIM).astype(jnp.int32)
            key_rows = lax.dynamic_slice_in_dim(seq_keys, kv_start, HEAD_DIM, 1)
            value_rows = lax.dynamic_slice_in_dim(seq_values, kv_start, HEAD_DIM, 1)
            return attend(query_rows, key_rows, value_rows)
        attended = lax.map(one_head, jnp.arange(HEADS, dtype=jnp.int32))
        attended = jnp.transpose(attended, (1, 0, 2)).reshape(SEQ, HEADS * HEAD_DIM)
        act_scaled = quantize(attended, act_exponent)
        grad_scaled = quantize(seq_grad.astype(jnp.float32), grad_exponent)
        seq_partial = lax.dot_general(grad_scaled, act_scaled, (((0,), (0,)), ((), ())), preferred_element_type=jnp.float32)
        seq_partial = (seq_partial * dequant).astype(jnp.bfloat16)
        return (running + seq_partial.astype(jnp.float32), None)
    zero_sum = jnp.zeros((D, HEADS * HEAD_DIM), jnp.float32)
    grad_weight, unused = lax.scan(sequence_grad, zero_sum, jnp.arange(N_DP, dtype=jnp.int32))
    return grad_weight
```

```python
import functools

import jax
import jax.numpy as jnp
from jax import lax
from jax.experimental import pallas as pl
from jax.experimental.pallas import tpu as pltpu
from jax.sharding import PartitionSpec as P

HEAD_DIM = 128
SATURATION = 448.0
NY, NZ, NC, NX = 2, 4, 2, 4
AXES = ("dp", "tensor")
UNITS = 4
ROWS = 128


def device_of(yh, z, c, yl, x):
    return ((yh * NZ + z) * NC + c) * (NY * NX) + yl * NX + x


def pairs_of(target):
    pairs = []
    for yh in range(NY):
        for z in range(NZ):
            for c in range(NC):
                for yl in range(NY):
                    for x in range(NX):
                        pairs.append((device_of(yh, z, c, yl, x), device_of(*target(yh, z, c, yl, x))))
    return pairs


X_UP = pairs_of(lambda yh, z, c, yl, x: (yh, z, c, yl, (x + 1) % NX))
X_DOWN = pairs_of(lambda yh, z, c, yl, x: (yh, z, c, yl, (x - 1) % NX))
Z_UP = pairs_of(lambda yh, z, c, yl, x: (yh, (z + 1) % NZ, c, yl, x))
Z_DOWN = pairs_of(lambda yh, z, c, yl, x: (yh, (z - 1) % NZ, c, yl, x))
Y_INNER = pairs_of(lambda yh, z, c, yl, x: (yh, z, c, 1 - yl, x))
Y_OUTER = pairs_of(lambda yh, z, c, yl, x: (1 - yh, z, c, 1 - yl, x))
CORES = pairs_of(lambda yh, z, c, yl, x: (yh, z, 1 - c, yl, x))


def send(block, pairs):
    return lax.ppermute(block, AXES, pairs)


def quantize_kernel(columns, factor_ref, grad_ref, out_ref, *, base):
    part = pl.program_id(0)
    for unit in range(UNITS):
        for step in range(NZ):
            column = columns[(base + part) * (UNITS * NZ) + unit * NZ + step]
            block = grad_ref[:, pl.ds(pl.multiple_of(column * ROWS, ROWS), ROWS)].astype(jnp.float32)
            scaled = jnp.clip(block * factor_ref[0], -SATURATION, SATURATION)
            out_ref[0, unit, step * ROWS : (step + 1) * ROWS, :] = scaled.T.astype(jnp.bfloat16)


def quantize_columns(columns, factor, out_grad, base):
    tokens, width = out_grad.shape
    return pl.pallas_call(
        functools.partial(quantize_kernel, base=base),
        grid_spec=pltpu.PrefetchScalarGridSpec(
            num_scalar_prefetch=2,
            grid=(2,),
            in_specs=[pl.BlockSpec((tokens, width), lambda i, *_: (0, 0))],
            out_specs=pl.BlockSpec((1, UNITS, NZ * ROWS, tokens), lambda i, *_: (i, 0, 0, 0)),
        ),
        out_shape=jax.ShapeDtypeStruct((2, UNITS, NZ * ROWS, tokens), jnp.bfloat16),
    )(columns, factor, out_grad)


Q_BLOCK = 256


def attention_kernel(places, factor_ref, query_ref, key_ref, value_ref, *rest):
    out_ref = rest[-1]
    seq_len = key_ref.shape[0]
    scale = HEAD_DIM**-0.5
    for start in range(0, seq_len, Q_BLOCK):
        seen = start + Q_BLOCK
        scores = lax.dot_general(
            query_ref[start:seen, :],
            key_ref[:seen, :],
            (((1,), (1,)), ((), ())),
            preferred_element_type=jnp.float32,
        )
        row = lax.broadcasted_iota(jnp.int32, scores.shape, 0) + start
        column = lax.broadcasted_iota(jnp.int32, scores.shape, 1)
        scores = jnp.where(column <= row, scores, jnp.float32(-1e30))
        row_max = jnp.max(scores, axis=1, keepdims=True)
        weights = jnp.exp((scores - row_max) * scale)
        total = jnp.sum(weights, axis=1, keepdims=True)
        mixed = jnp.dot(weights.astype(jnp.bfloat16), value_ref[:seen, :], preferred_element_type=jnp.float32)
        attended = mixed / total
        scaled = jnp.clip(attended * factor_ref[0], -SATURATION, SATURATION).astype(jnp.bfloat16)
        for part in range(Q_BLOCK // ROWS):
            place = places[start // ROWS + part]
            out_ref[pl.ds(place, 1)] = scaled[part * ROWS : (part + 1) * ROWS][None]


def attend(places, factor, queries, keys, values, first, heads, carried):
    seq_len, width = queries.shape
    blocks = seq_len // ROWS
    in_specs = [
        pl.BlockSpec((seq_len, HEAD_DIM), lambda h, *_: (0, h + first)),
        pl.BlockSpec((seq_len, HEAD_DIM), lambda h, *_: (0, 0)),
        pl.BlockSpec((seq_len, HEAD_DIM), lambda h, *_: (0, 0)),
    ]
    operands = [places, factor, queries, keys, values]
    aliases = {}
    if carried is not None:
        in_specs.append(pl.BlockSpec(memory_space=pl.ANY))
        aliases = {len(operands): 0}
        operands.append(carried)
    return pl.pallas_call(
        attention_kernel,
        grid_spec=pltpu.PrefetchScalarGridSpec(
            num_scalar_prefetch=2,
            grid=(heads,),
            in_specs=in_specs,
            out_specs=pl.BlockSpec((blocks, ROWS, HEAD_DIM), lambda h, *_: (0, 0, h + first)),
        ),
        out_shape=jax.ShapeDtypeStruct((blocks, ROWS, width), jnp.bfloat16),
        input_output_aliases=aliases,
    )(*operands)


COLUMN_BLOCK = 256


def product_kernel(*refs, sides):
    own_x, left, right, far_first, far_second = refs[:5]
    acts = refs[5 : 5 + 2 * len(sides)]
    far_a, far_b, up, down, own = refs[5 + 2 * len(sides) : -1]
    grads = refs[-1]
    column = pl.program_id(1)

    @pl.when(column == 0)
    def _():
        for seq in range(2):
            for source, piece in enumerate((own_x, left, right, far_first if seq == 0 else far_second)):
                for row in range(2):
                    at = ((seq * NX + source) * 2 + row) * ROWS
                    block = piece[0, row] if source == 3 else piece[0, seq, row]
                    grads[:, at : at + ROWS] = block

    half = grads.shape[1] // 2

    def product(first, second):
        tile = jnp.dot(grads[:, :half], first[...].reshape(half, COLUMN_BLOCK), preferred_element_type=jnp.float32)
        tile = tile + jnp.dot(grads[:, half:], second[...].reshape(half, COLUMN_BLOCK), preferred_element_type=jnp.float32)
        far_a[0] = tile[: ROWS // 2].astype(far_a.dtype)
        far_b[0] = tile[ROWS // 2 : ROWS].astype(far_b.dtype)
        up[0] = tile[ROWS : 2 * ROWS].astype(up.dtype)
        down[0] = tile[2 * ROWS : 3 * ROWS].astype(down.dtype)
        own[0] = tile[3 * ROWS :].astype(own.dtype)

    if len(sides) == 1:
        product(acts[0], acts[1])
    else:
        split = sides[0]

        @pl.when(column < split)
        def _():
            product(acts[0], acts[1])

        @pl.when(column >= split)
        def _():
            product(acts[2], acts[3])


def products(pieces, acts, ranges):
    own_x, left, right, far_first, far_second = pieces
    units = own_x.shape[0]
    tokens = own_x.shape[-1]
    counts = [stop - start for start, stop in ranges]
    columns = sum(counts)
    width = columns * COLUMN_BLOCK
    whole = lambda a: pl.BlockSpec((1,) + a.shape[1:], lambda u, j: (u,) + (0,) * (a.ndim - 1))
    in_specs = [whole(a) for a in pieces]
    operands = list(pieces)
    before = 0
    for pair, (start, stop) in zip(acts, ranges, strict=True):
        for a in pair:
            in_specs.append(
                pl.BlockSpec(
                    (a.shape[0], a.shape[1], COLUMN_BLOCK),
                    lambda u, j, start=start, stop=stop, before=before: (0, 0, jnp.clip(j - before + start, start, stop - 1)),
                )
            )
            operands.append(a)
        before += stop - start
    shapes = [(ROWS // 2, jnp.bfloat16)] * 2 + [(ROWS, jnp.bfloat16)] * 2 + [(ROWS, jnp.float32)]
    return pl.pallas_call(
        functools.partial(product_kernel, sides=tuple(counts)),
        grid=(units, columns),
        in_specs=in_specs,
        out_specs=[pl.BlockSpec((1, r, COLUMN_BLOCK), lambda u, j: (u, 0, j)) for r, _ in shapes],
        out_shape=[jax.ShapeDtypeStruct((units, r, width), d) for r, d in shapes],
        scratch_shapes=[pltpu.VMEM((NZ * ROWS, 4 * NX * tokens), jnp.bfloat16)],
        compiler_params=pltpu.CompilerParams(dimension_semantics=("arbitrary", "arbitrary")),
    )(*operands)


def reduce_over_z(parts):
    far_a, far_b, up, down, own = parts
    from_below = send(far_a, Z_UP)
    from_above = send(far_b, Z_DOWN)
    half = ROWS // 2
    f32 = jnp.float32
    up = jnp.concatenate([(up[:, :half].astype(f32) + from_below.astype(f32)).astype(up.dtype), up[:, half:]], 1)
    down = jnp.concatenate([down[:, :half], (down[:, half:].astype(f32) + from_above.astype(f32)).astype(down.dtype)], 1)
    first = send(up, Z_UP)
    second = send(down, Z_DOWN)
    return own + first.astype(f32) + second.astype(f32)


HEAD_GROUPS = ((0, 2), (2, 2), (4, 2), (6, 2))


def on_device(saved_queries, saved_keys, saved_values, out_grad, act_exponent, grad_exponent):
    f32 = jnp.float32
    place = lax.axis_index("dp")
    side = lax.axis_index("tensor")
    yh, z, c = place // (NZ * NC), place // NC % NZ, place % NC
    yl, x = side // NX, side % NX
    q = yl ^ yh
    act_factor = SATURATION * jnp.exp2(-act_exponent.astype(f32))
    grad_factor = SATURATION * jnp.exp2(-grad_exponent.astype(f32))
    dequant = jnp.exp2((act_exponent[0] + grad_exponent[0]).astype(f32)) / (SATURATION * SATURATION)

    core_at = jnp.arange(2)[:, None, None, None, None] ^ c
    chip_at = jnp.arange(2)[None, :, None, None, None] ^ q
    half_at = jnp.arange(2)[None, None, :, None, None]
    yh_at = jnp.array([1, 0])[None, None, None, :, None] ^ yh
    z_at = (jnp.array([2, 1, 3, 0])[None, None, None, None, :] + z) % NZ
    order = 4 * (8 * yh_at + 2 * z_at + chip_at) + 2 * core_at + half_at
    order = order.reshape(-1).astype(jnp.int32)
    token_y = jnp.arange(8) // NX
    token_x = jnp.arange(8) % NX
    places = (jnp.array([0, 2, 3, 1])[(token_x - x) % NX] * 2 + (token_y ^ yl)).astype(jnp.int32)

    for_other_core = quantize_columns(order, grad_factor, out_grad, 2)
    from_other_core = send(for_other_core, CORES)
    mine = quantize_columns(order, grad_factor, out_grad, 0)

    to_y = jnp.stack([mine[1], from_other_core[1]], axis=1)
    y_first = send(to_y[:1], Y_INNER)
    y_rest = send(to_y[1:], Y_INNER)
    pieces = []
    for unit in range(UNITS):
        from_y = y_first[0] if unit == 0 else y_rest[unit - 1]
        block = jnp.stack([mine[0, unit], from_y[0], from_other_core[0, unit], from_y[1]], 0)
        block = block.reshape((1, 2, 2) + block.shape[1:])
        left = send(block, X_UP)
        right = send(block, X_DOWN)
        far_first = send(left[:, 0], X_UP)
        far_second = send(right[:, 1], X_DOWN)
        pieces.append((block, left, right, far_first, far_second))

    acts = None
    for first, heads in HEAD_GROUPS:
        acts = attend(places, act_factor, saved_queries, saved_keys, saved_values, first, heads, acts)
    acts_other = send(acts, CORES)
    acts_y = send(acts, Y_INNER)
    flip = lambda a: a.reshape((NX, 2) + a.shape[1:])[:, ::-1].reshape(a.shape)
    acts_y = flip(acts_y)
    acts_y_other = send(acts_y, CORES)
    own_pair, y_pair = (acts, acts_other), (acts_y, acts_y_other)

    own_sums = [None] * UNITS
    y_sums = [None] * UNITS
    for unit in range(3):
        own_sums[unit] = reduce_over_z(products(pieces[unit], [own_pair], [(0, 4)]))
    for unit in range(3):
        y_sums[unit] = reduce_over_z(products(pieces[unit], [y_pair], [(0, 4)]))
    last = reduce_over_z(products(pieces[3], [own_pair, y_pair], [(0, 4), (0, 4)]))
    own_sums[3], y_sums[3] = last[..., :1024], last[..., 1024:]

    blocks = []
    for half in range(2):
        other, near = 2 * half, 2 * half + 1
        outgoing = jnp.concatenate([own_sums[other], y_sums[other]], -1).astype(jnp.bfloat16)
        incoming = send(outgoing, Y_OUTER).astype(f32)
        total_own = own_sums[near] + incoming[..., 1024:]
        total_y = (y_sums[near] + incoming[..., :1024]).astype(jnp.bfloat16)
        swapped = send(total_y, Y_INNER)
        stays = q == c
        keep = jnp.where(stays, total_own, swapped.astype(f32))
        give = jnp.where(stays, swapped, total_own.astype(jnp.bfloat16))
        given = send(give, CORES).astype(f32)
        blocks.append((keep, given))
    keep = jnp.concatenate([b[0] for b in blocks], 0)
    given = jnp.concatenate([b[1] for b in blocks], 0)
    result = jnp.where(c == 0, jnp.stack([keep, given]), jnp.stack([given, keep])) * dequant
    return result.reshape(4 * ROWS, -1)


def solution(mesh):
    in_specs = (
        P("dp", "tensor"),
        P("dp", "tensor"),
        P("dp", "tensor"),
        P(("dp", "tensor"), None),
        P(),
        P(),
    )
    out_specs = P("dp", "tensor")
    return jax.shard_map(
        on_device, mesh=mesh, in_specs=in_specs, out_specs=out_specs, check_vma=False
    )
```

```python
import functools

import jax
import jax.numpy as jnp
from jax import lax
from jax.experimental import pallas as pl
from jax.experimental.pallas import tpu as pltpu
from jax.sharding import PartitionSpec as P


HEAD_DIM = 128
SATURATION = 448.0
NY, NZ, NC, NX = 2, 4, 2, 4
AXES = ("dp", "tensor")
UNITS = 4
ROWS = 128
STEPS = (2, 1, 3, 0)
QUARTER = 256


def device_of(yh, z, c, yl, x):
    return ((yh * NZ + z) * NC + c) * (NY * NX) + yl * NX + x


def pairs_of(target):
    pairs = []
    for yh in range(NY):
        for z in range(NZ):
            for c in range(NC):
                for yl in range(NY):
                    for x in range(NX):
                        pairs.append((device_of(yh, z, c, yl, x), device_of(*target(yh, z, c, yl, x))))
    return pairs


X_UP = pairs_of(lambda yh, z, c, yl, x: (yh, z, c, yl, (x + 1) % NX))
X_DOWN = pairs_of(lambda yh, z, c, yl, x: (yh, z, c, yl, (x - 1) % NX))
Z_UP = pairs_of(lambda yh, z, c, yl, x: (yh, (z + 1) % NZ, c, yl, x))
Z_DOWN = pairs_of(lambda yh, z, c, yl, x: (yh, (z - 1) % NZ, c, yl, x))
Y_INNER = pairs_of(lambda yh, z, c, yl, x: (yh, z, c, 1 - yl, x))
Y_OUTER = pairs_of(lambda yh, z, c, yl, x: (1 - yh, z, c, 1 - yl, x))
CORES = pairs_of(lambda yh, z, c, yl, x: (yh, z, 1 - c, yl, x))


def send(block, pairs):
    return lax.ppermute(block, AXES, pairs)


def position():
    place = lax.axis_index("dp")
    side = lax.axis_index("tensor")
    return place // (NZ * NC), place // NC % NZ, place % NC, side // NX, side % NX


def saturation_factor(exponent_ref, width):
    exponent = jnp.full((1, width), -exponent_ref[0].astype(jnp.float32))
    return SATURATION * jnp.exp2(exponent)


GROUPS = ((0, 1), (1, 1), (2, 2))
FIRST = ((1, 1, 0, 1), (0, 1, 0, 1), (1, 0, 0, 1), (0, 0, 0, 1))
REST = ((1, 0, 1, 3), (1, 1, 1, 1), (1, 1, 2, 2)) + tuple((0, 0, u, 1) for u in (1, 2, 3)) + ((0, 1, 1, 1), (0, 1, 2, 2))


def quantize_kernel(exponent_ref, grad_ref, *out_refs, made):
    yh, z, c, yl, _ = position()
    factor = saturation_factor(exponent_ref, ROWS)
    for (other_core, far_chip, first, count), ref in zip(made, out_refs, strict=True):
        chip = (yl ^ yh) ^ far_chip
        core = c ^ other_core
        for unit in range(first, first + count):
            for step in range(NZ):
                yh_at = yh if unit % 2 else 1 - yh
                z_at = lax.rem(z + STEPS[step], NZ)
                column = 4 * (8 * yh_at + 2 * z_at + chip) + 2 * core + unit // 2
                values = grad_ref[:, pl.ds(pl.multiple_of(column * ROWS, ROWS), ROWS)].astype(jnp.float32)
                scaled = jnp.clip(values * factor, -SATURATION, SATURATION).astype(jnp.bfloat16)
                ref[unit - first, step * ROWS : (step + 1) * ROWS, :] = scaled.T


def quantize_columns(exponent, out_grad, made):
    tokens = out_grad.shape[0]
    arrays = pl.pallas_call(
        functools.partial(quantize_kernel, made=made),
        in_specs=[pl.BlockSpec(memory_space=pltpu.SMEM), pl.BlockSpec(memory_space=pltpu.VMEM)],
        out_specs=[pl.BlockSpec(memory_space=pltpu.VMEM)] * len(made),
        out_shape=[jax.ShapeDtypeStruct((n, NZ * ROWS, tokens), jnp.bfloat16) for *_, n in made],
        cost_estimate=pl.CostEstimate(flops=2 * 10**9, bytes_accessed=3 * 2**20, transcendentals=0),
    )(exponent, out_grad)
    return dict(zip(made, arrays, strict=True))


Q_BLOCK = 256


def attention_kernel(exponent_ref, query_ref, key_ref, value_ref, out_ref):
    _, _, _, _, x = position()
    seq_len = key_ref.shape[0]
    scale = HEAD_DIM**-0.5
    factor = saturation_factor(exponent_ref, HEAD_DIM)
    row = lax.broadcasted_iota(jnp.int32, (Q_BLOCK, Q_BLOCK), 0)
    column = lax.broadcasted_iota(jnp.int32, (Q_BLOCK, Q_BLOCK), 1)
    causal = column <= row
    for start in range(0, seq_len, Q_BLOCK):
        queries = query_ref[start : start + Q_BLOCK, :]

        def scores_of(first, last):
            return lax.dot_general(
                queries, key_ref[first:last, :], (((1,), (1,)), ((), ())), preferred_element_type=jnp.float32
            )

        near = jnp.where(causal, scores_of(start, start + Q_BLOCK), jnp.float32(-1e30))
        row_max = jnp.max(near, axis=1, keepdims=True)
        if start:
            past = scores_of(0, start)
            row_max = jnp.maximum(row_max, jnp.max(past, axis=1, keepdims=True))
        weights = jnp.exp((near - row_max) * scale)
        total = jnp.sum(weights, axis=1, keepdims=True)
        mixed = jnp.dot(
            weights.astype(jnp.bfloat16), value_ref[start : start + Q_BLOCK, :], preferred_element_type=jnp.float32
        )
        if start:
            weights = jnp.exp((past - row_max) * scale)
            total = total + jnp.sum(weights, axis=1, keepdims=True)
            mixed = mixed + jnp.dot(
                weights.astype(jnp.bfloat16), value_ref[:start, :], preferred_element_type=jnp.float32
            )
        scaled = jnp.clip(mixed / total * factor, -SATURATION, SATURATION).astype(jnp.bfloat16)
        for part in range(Q_BLOCK // ROWS):
            token_block = start // ROWS + part
            ahead = lax.rem(token_block % NX - x + NX, NX)
            order = jnp.where(ahead == 0, 0, jnp.where(ahead == 3, 1, ahead + 1))
            out_ref[pl.ds(order * 2 + token_block // NX, 1)] = scaled[part * ROWS : (part + 1) * ROWS][None]


def attend(exponent, queries, keys, values, first, heads):
    seq_len = queries.shape[0]
    blocks = seq_len // ROWS
    return pl.pallas_call(
        attention_kernel,
        grid=(heads,),
        in_specs=[
            pl.BlockSpec(memory_space=pltpu.SMEM),
            pl.BlockSpec((seq_len, HEAD_DIM), lambda h: (0, h + first)),
            pl.BlockSpec((seq_len, HEAD_DIM), lambda h: (0, 0)),
            pl.BlockSpec((seq_len, HEAD_DIM), lambda h: (0, 0)),
        ],
        out_specs=pl.BlockSpec((blocks, ROWS, HEAD_DIM), lambda h: (0, 0, h)),
        out_shape=jax.ShapeDtypeStruct((blocks, ROWS, heads * HEAD_DIM), jnp.bfloat16),
        cost_estimate=pl.CostEstimate(flops=4 * 10**9, bytes_accessed=2**20, transcendentals=0),
    )(exponent, queries, keys, values)


def product_kernel(*refs, jobs, units, acts):
    piece_refs = [refs[4 * u : 4 * u + 4] for u in range(units)]
    act_refs = [refs[4 * units + 2 * a : 4 * units + 2 * a + 2] for a in range(acts // 2)]
    outs = refs[4 * units + acts : 4 * units + acts + 4]
    grads, values, results, grad_sem, value_sem, result_sem = refs[4 * units + acts + 4 :]
    yl = position()[3]
    grad_copies = []
    for u in range(units):
        for seq in range(2):
            for source in range(NX):
                for row in range(2):
                    at = (seq * NX + source) * 2 + row
                    grad_copies.append(
                        pltpu.make_async_copy(
                            piece_refs[u][source].at[seq, row ^ yl],
                            grads.at[u, :, pl.ds(at * ROWS, ROWS)],
                            grad_sem.at[u, at],
                        )
                    )
    value_copies = [
        pltpu.make_async_copy(
            act_refs[a // 2][seq].at[:, :, pl.ds(a % 2 * QUARTER, QUARTER)], values.at[a, seq], value_sem.at[a, seq]
        )
        for a in range(acts)
        for seq in range(2)
    ]
    per_unit = len(grad_copies) // units
    for copy in grad_copies[:per_unit] + value_copies + grad_copies[per_unit:]:
        copy.start()
    waited = 0
    done = 0
    for u in range(units):
        for copy in grad_copies[u * per_unit : (u + 1) * per_unit]:
            copy.wait()
        for first, count, out_first in jobs[u]:

            def step(j, carry, u=u, first=first, out_first=out_first, waited=waited):
                @pl.when(first + j >= waited)
                def _():
                    for seq in range(2):
                        pltpu.make_async_copy(
                            act_refs[0][seq].at[:, :, pl.ds(0, QUARTER)],
                            values.at[first + j, seq],
                            value_sem.at[first + j, seq],
                        ).wait()

                act = values[first + j].reshape(-1, QUARTER)
                tile = jnp.dot(grads[u], act, preferred_element_type=jnp.float32)
                at = out_first + j
                results[at] = tile.astype(results.dtype)
                for part in range(NZ):
                    pltpu.make_async_copy(
                        results.at[at, pl.ds(part * ROWS, ROWS), :],
                        outs[part].at[:, pl.ds(pl.multiple_of(at * QUARTER, QUARTER), QUARTER)],
                        result_sem.at[at, part],
                    ).start()
                return carry

            lax.fori_loop(0, count, step, 0)
            waited = max(waited, first + count)
            done += count

    def settle(at, carry):
        for part in range(NZ):
            pltpu.make_async_copy(
                results.at[at, pl.ds(part * ROWS, ROWS), :],
                outs[part].at[:, pl.ds(pl.multiple_of(at * QUARTER, QUARTER), QUARTER)],
                result_sem.at[at, part],
            ).wait()
        return carry

    lax.fori_loop(0, done, settle, 0)


def products(pieces, acts, jobs):
    units, count = len(pieces), 2 * len(acts)
    total = sum(n for runs in jobs for _, n, _ in runs)
    operands = [a for piece in pieces for a in piece] + [a for pair in acts for a in pair]
    tokens = pieces[0][0].shape[-1]
    shape = acts[0][0].shape[:2] + (QUARTER,)
    flops = 2 * total * QUARTER * NZ * ROWS * 2 * shape[0] * shape[1]
    return pl.pallas_call(
        functools.partial(product_kernel, jobs=jobs, units=units, acts=count),
        in_specs=[pl.BlockSpec(memory_space=pl.ANY)] * len(operands),
        out_specs=[pl.BlockSpec(memory_space=pl.ANY)] * NZ,
        out_shape=[jax.ShapeDtypeStruct((ROWS, total * QUARTER), jnp.bfloat16)] * NZ,
        scratch_shapes=[
            pltpu.VMEM((units, NZ * ROWS, 4 * NX * tokens), jnp.bfloat16),
            pltpu.VMEM((count, 2) + shape, jnp.bfloat16),
            pltpu.VMEM((total, NZ * ROWS, QUARTER), jnp.bfloat16),
            pltpu.SemaphoreType.DMA((units, 4 * NX)),
            pltpu.SemaphoreType.DMA((count, 2)),
            pltpu.SemaphoreType.DMA((total, NZ)),
        ],
        cost_estimate=pl.CostEstimate(flops=flops, bytes_accessed=2**20, transcendentals=0),
    )(*operands)


def reduce_over_z(parts, upward, hold):
    f32 = jnp.float32
    far, up, down, own = parts
    passing = send(far, Z_UP if upward else Z_DOWN)
    if hold is not None:
        passing, _ = lax.optimization_barrier((passing, hold))
    if upward:
        below_sent = send((up.astype(f32) + passing.astype(f32)).astype(up.dtype), Z_UP)
        above_sent = send(down, Z_DOWN)
    else:
        above_sent = send((down.astype(f32) + passing.astype(f32)).astype(down.dtype), Z_DOWN)
        below_sent = send(up, Z_UP)
    return own, below_sent, above_sent


HEADS_PER_HALF = 2 * QUARTER // HEAD_DIM

PORTIONS = (
    ("pa", ((0, "own", 0, 4),)),
    ("pb", ((0, "y", 0, 2), (1, "own", 0, 4), (1, "y", 0, 2))),
    ("pc", ((0, "y", 2, 2), (1, "y", 2, 2))),
    ("pd", ((2, "own", 0, 4), (2, "y", 0, 4))),
    ("pe", ((3, "own", 0, 4), (3, "y", 0, 4))),
)
OUTER = (("pa", "pb", "pc"), ("pd",))


def program(saved_queries, saved_keys, saved_values, out_grad, act_exponent, grad_exponent):
    f32, bf16 = jnp.float32, jnp.bfloat16
    yh, _, c, yl, _ = position()
    chip = yl ^ yh
    dequant = jnp.exp2((act_exponent[0] + grad_exponent[0]).astype(f32)) / (SATURATION * SATURATION)

    blocks = quantize_columns(grad_exponent, out_grad, FIRST)
    blocks |= quantize_columns(grad_exponent, out_grad, REST)
    near_sent = [send(blocks[1, 0, *group], CORES) for group in ((0, 1), (1, 3))]
    theirs = [near_sent[0][0], *(near_sent[1][i] for i in range(3))]
    mine = [blocks[0, 0, unit, 1][0] for unit in range(UNITS)]

    acts = {}
    for half in range(2):
        a = attend(act_exponent, saved_queries, saved_keys, saved_values, half * HEADS_PER_HALF, HEADS_PER_HALF)
        acts["own", half] = (a, send(a, CORES))
        b = send(a, Y_INNER)
        acts["y", half] = (b, send(b, CORES))

    from_y = {}
    for first, count in GROUPS:
        near = send(blocks[0, 1, first, count], Y_INNER)
        other = send(send(blocks[1, 1, first, count], CORES), Y_INNER)
        if count > 1:
            near, other, _ = lax.optimization_barrier((near, other, acts["own", 1][0]))
        for unit in range(first, first + count):
            from_y[unit] = (near[unit - first], other[unit - first])

    pieces = []
    for unit in range(UNITS):
        block = jnp.stack([mine[unit], from_y[unit][0], theirs[unit], from_y[unit][1]])
        block = block.reshape((2, 2) + block.shape[1:])
        left = send(block, X_UP)
        right = send(block, X_DOWN)
        far = send(left, X_UP) if unit % 2 == 0 else send(right, X_DOWN)
        pieces.append((block, left, right, far))

    made = {}
    for name, runs in PORTIONS:
        units, used, jobs, at = [], [], [], 0
        for unit, side, first, count in runs:
            if unit not in units:
                units.append(unit)
                jobs.append([])
            for quarter in range(first, first + count):
                if (side, quarter) not in used:
                    used.append((side, quarter))
            jobs[units.index(unit)].append((used.index((side, first)), count, at))
            at += count
        halves = [acts[side, quarter // 2] for side, quarter in used[::2]]
        made[name] = products([pieces[u] for u in units], halves, jobs)

    sums = {}
    leaving = {}
    for index, (name, runs) in enumerate(PORTIONS):
        later = made[PORTIONS[index + 1][0]][3] if index + 1 < len(PORTIONS) else None
        own, below, above = reduce_over_z(made[name], index % 2 == 0, later)
        at = 0
        leaving[name] = []
        for unit, side, first, count in runs:
            for k in range(count):
                sums[unit, side, first + k] = (own, below, above, at)
                if unit % 2 == 0:
                    leaving[name].append((unit, side, first + k))
                at += 1

    outgoing, out_places = {}, []
    for index, names in enumerate(OUTER):
        at, columns = 0, []
        for name in names:
            cut = len(leaving[name]) * QUARTER
            own, below, above, _ = sums[leaving[name][0]]
            if index == 0:
                own, below, above, _ = lax.optimization_barrier((own, below, above, made["pe"][3]))
            columns.append(own[:, :cut].astype(f32) + below[:, :cut].astype(f32) + above[:, :cut].astype(f32))
            for key in leaving[name]:
                out_places.append((*key, index, at))
                at += 1
        message = jnp.concatenate(columns, 1).astype(bf16)
        outgoing[index] = send(message, Y_OUTER)
        if index:
            outgoing[0], _ = lax.optimization_barrier((outgoing[0], message))

    incoming = {}
    for unit, side, quarter, name, at in out_places:
        incoming[unit + 1, "y" if side == "own" else "own", quarter] = (outgoing[name], at)

    def total(unit, side, hold=None):
        columns = []
        for quarter in range(4):
            own, below, above, at = sums[unit, side, quarter]
            arrived, there = incoming[unit, side, quarter]
            if hold is not None:
                own, below, above, arrived, _ = lax.optimization_barrier((own, below, above, arrived, hold))
            cut = slice(at * QUARTER, (at + 1) * QUARTER)
            columns.append(
                own[:, cut].astype(f32)
                + below[:, cut].astype(f32)
                + above[:, cut].astype(f32)
                + arrived[:, there * QUARTER : (there + 1) * QUARTER].astype(f32)
            )
        return jnp.concatenate(columns, 1)

    keeps, gifts = [], []
    for half in range(2):
        unit = 2 * half + 1
        leaves = total(unit, "y").astype(bf16)
        swapped = send(leaves, Y_INNER)
        near = total(unit, "own", leaves)
        stays = chip == c
        keeps.append(jnp.where(stays, near, swapped.astype(f32)))
        gifts.append(send(jnp.where(stays, swapped, near.astype(bf16)), CORES).astype(f32))
    keep, gift = jnp.concatenate(keeps, 0), jnp.concatenate(gifts, 0)
    result = jnp.where(c == 0, jnp.stack([keep, gift]), jnp.stack([gift, keep])) * dequant
    return result.reshape(4 * ROWS, -1)


def solution(mesh):
    in_specs = (
        P("dp", "tensor"),
        P("dp", "tensor"),
        P("dp", "tensor"),
        P(("dp", "tensor"), None),
        P(),
        P(),
    )
    out_specs = P("dp", "tensor")
    return jax.shard_map(program, mesh=mesh, in_specs=in_specs, out_specs=out_specs, check_vma=False)
```

```python
import functools

import jax
import jax.numpy as jnp
from jax import lax
from jax.experimental import pallas as pl
from jax.experimental.pallas import tpu as pltpu
from jax.sharding import PartitionSpec as P


HEAD_DIM = 128
SATURATION = 448.0
NY, NZ, NC, NX = 2, 4, 2, 4
AXES = ("dp", "tensor")
UNITS = 4
ROWS = 128
STEPS = (2, 1, 3, 0)
QUARTER = 256
AHEAD = 2


def device_of(yh, z, c, yl, x):
    return ((yh * NZ + z) * NC + c) * (NY * NX) + yl * NX + x


def pairs_of(target):
    pairs = []
    for yh in range(NY):
        for z in range(NZ):
            for c in range(NC):
                for yl in range(NY):
                    for x in range(NX):
                        pairs.append((device_of(yh, z, c, yl, x), device_of(*target(yh, z, c, yl, x))))
    return pairs


X_UP = pairs_of(lambda yh, z, c, yl, x: (yh, z, c, yl, (x + 1) % NX))
X_DOWN = pairs_of(lambda yh, z, c, yl, x: (yh, z, c, yl, (x - 1) % NX))
Z_UP = pairs_of(lambda yh, z, c, yl, x: (yh, (z + 1) % NZ, c, yl, x))
Z_DOWN = pairs_of(lambda yh, z, c, yl, x: (yh, (z - 1) % NZ, c, yl, x))
Y_INNER = pairs_of(lambda yh, z, c, yl, x: (yh, z, c, 1 - yl, x))
Y_OUTER = pairs_of(lambda yh, z, c, yl, x: (1 - yh, z, c, 1 - yl, x))
CORES = pairs_of(lambda yh, z, c, yl, x: (yh, z, 1 - c, yl, x))


def send(block, pairs):
    return lax.ppermute(block, AXES, pairs)


def position():
    place = lax.axis_index("dp")
    side = lax.axis_index("tensor")
    return place // (NZ * NC), place // NC % NZ, place % NC, side // NX, side % NX


def saturation_factor(exponent_ref, width):
    exponent = jnp.full((1, width), -exponent_ref[0].astype(jnp.float32))
    return SATURATION * jnp.exp2(exponent)


GROUPS = ((0, 1), (1, 1), (2, 2))
FIRST = ((1, 1, 0, 1), (0, 1, 0, 1), (1, 0, 0, 1), (0, 0, 0, 1))
REST = ((1, 0, 1, 3), (1, 1, 1, 1), (1, 1, 2, 2)) + tuple((0, 0, u, 1) for u in (1, 2, 3)) + ((0, 1, 1, 1), (0, 1, 2, 2))


def quantize_kernel(exponent_ref, grad_ref, *out_refs, made):
    yh, z, c, yl, _ = position()
    factor = saturation_factor(exponent_ref, ROWS)
    for (other_core, far_chip, first, count), ref in zip(made, out_refs, strict=True):
        chip = (yl ^ yh) ^ far_chip
        core = c ^ other_core
        for unit in range(first, first + count):
            for step in range(NZ):
                yh_at = yh if unit % 2 else 1 - yh
                z_at = lax.rem(z + STEPS[step], NZ)
                column = 4 * (8 * yh_at + 2 * z_at + chip) + 2 * core + unit // 2
                values = grad_ref[:, pl.ds(pl.multiple_of(column * ROWS, ROWS), ROWS)].astype(jnp.float32)
                scaled = jnp.clip(values * factor, -SATURATION, SATURATION).astype(jnp.bfloat16)
                ref[unit - first, step * ROWS : (step + 1) * ROWS, :] = scaled.T


def quantize_columns(exponent, out_grad, made):
    tokens = out_grad.shape[0]
    arrays = pl.pallas_call(
        functools.partial(quantize_kernel, made=made),
        in_specs=[pl.BlockSpec(memory_space=pltpu.SMEM), pl.BlockSpec(memory_space=pltpu.VMEM)],
        out_specs=[pl.BlockSpec(memory_space=pltpu.VMEM)] * len(made),
        out_shape=[jax.ShapeDtypeStruct((n, NZ * ROWS, tokens), jnp.bfloat16) for *_, n in made],
        cost_estimate=pl.CostEstimate(flops=2 * 10**9, bytes_accessed=3 * 2**20, transcendentals=0),
    )(exponent, out_grad)
    return dict(zip(made, arrays, strict=True))


Q_BLOCK = 256
LOG2_E = 1.4426950408889634


def attention_kernel(exponent_ref, query_ref, key_ref, value_ref, out_ref):
    _, _, _, _, x = position()
    seq_len = key_ref.shape[0]
    scale = HEAD_DIM**-0.5 * LOG2_E
    factor = saturation_factor(exponent_ref, HEAD_DIM)
    row = lax.broadcasted_iota(jnp.int32, (Q_BLOCK, Q_BLOCK), 0)
    column = lax.broadcasted_iota(jnp.int32, (Q_BLOCK, Q_BLOCK), 1)
    causal = column <= row

    def scores_of(start):
        queries = query_ref[start : start + Q_BLOCK, :]

        def block(first, last):
            return lax.dot_general(
                queries, key_ref[first:last, :], (((1,), (1,)), ((), ())), preferred_element_type=jnp.float32
            )

        return block(start, start + Q_BLOCK), block(0, start) if start else None

    def weights_of(near, past):
        near = jnp.where(causal, near, jnp.float32(-1e30))
        row_max = jnp.max(near, axis=1, keepdims=True)
        if past is not None:
            row_max = jnp.maximum(row_max, jnp.max(past, axis=1, keepdims=True))
        near = jnp.exp2((near - row_max) * scale)
        total = jnp.sum(near, axis=1, keepdims=True)
        if past is not None:
            past = jnp.exp2((past - row_max) * scale)
            total = total + jnp.sum(past, axis=1, keepdims=True)
            past = past.astype(jnp.bfloat16)
        return near.astype(jnp.bfloat16), past, total

    def finish(start, near, past, total):
        mixed = jnp.dot(near, value_ref[start : start + Q_BLOCK, :], preferred_element_type=jnp.float32)
        if past is not None:
            mixed = mixed + jnp.dot(past, value_ref[:start, :], preferred_element_type=jnp.float32)
        scaled = jnp.clip(mixed / total * factor, -SATURATION, SATURATION).astype(jnp.bfloat16)
        for part in range(Q_BLOCK // ROWS):
            token_block = start // ROWS + part
            ahead = lax.rem(token_block % NX - x + NX, NX)
            order = jnp.where(ahead == 0, 0, jnp.where(ahead == 3, 1, ahead + 1))
            out_ref[pl.ds(order * 2 + token_block // NX, 1)] = scaled[part * ROWS : (part + 1) * ROWS][None]

    scores, waiting = scores_of(0), None
    for start in range(0, seq_len, Q_BLOCK):
        following = scores_of(start + Q_BLOCK) if start + Q_BLOCK < seq_len else None
        weights = weights_of(*scores)
        if waiting is not None:
            finish(*waiting)
        waiting, scores = (start, *weights), following
    finish(*waiting)


def attend(exponent, queries, keys, values, first, heads):
    seq_len = queries.shape[0]
    blocks = seq_len // ROWS
    return pl.pallas_call(
        attention_kernel,
        grid=(heads,),
        in_specs=[
            pl.BlockSpec(memory_space=pltpu.SMEM),
            pl.BlockSpec((seq_len, HEAD_DIM), lambda h: (0, h + first)),
            pl.BlockSpec((seq_len, HEAD_DIM), lambda h: (0, 0)),
            pl.BlockSpec((seq_len, HEAD_DIM), lambda h: (0, 0)),
        ],
        out_specs=pl.BlockSpec((blocks, ROWS, HEAD_DIM), lambda h: (0, 0, h)),
        out_shape=jax.ShapeDtypeStruct((blocks, ROWS, heads * HEAD_DIM), jnp.bfloat16),
        cost_estimate=pl.CostEstimate(flops=4 * 10**9, bytes_accessed=2**20, transcendentals=0),
    )(exponent, queries, keys, values)


def product_kernel(*refs, jobs, units, acts, extra, whole):
    piece_refs = [refs[4 * u : 4 * u + 4] for u in range(units)]
    act_refs = [refs[4 * units + 2 * a : 4 * units + 2 * a + 2] for a in range(acts // 2)]
    refs = refs[4 * units + acts :]
    extra_refs, refs = refs[:extra], refs[extra:]
    if whole:
        outs = [refs[0].at[pl.ds(part * ROWS, ROWS), :] for part in range(NZ)]
    else:
        outs = refs[:NZ]
    grads, values, results, grad_sem, value_sem, result_sem, *added = refs[1 if whole else NZ :]
    extra_copies = [pltpu.make_async_copy(ref, added[0], added[1].at[0]) for ref in extra_refs]
    yl = position()[3]
    grad_copies = []
    for u in range(units):
        for seq in range(2):
            for source in range(NX):
                for row in range(2):
                    at = (seq * NX + source) * 2 + row
                    grad_copies.append(
                        pltpu.make_async_copy(
                            piece_refs[u][source].at[seq, row ^ yl],
                            grads.at[u, :, pl.ds(at * ROWS, ROWS)],
                            grad_sem.at[u, at],
                        )
                    )
    value_copies = [
        pltpu.make_async_copy(
            act_refs[a // 2][seq].at[:, :, pl.ds(a % 2 * QUARTER, QUARTER)], values.at[a, seq], value_sem.at[a, seq]
        )
        for a in range(acts)
        for seq in range(2)
    ]
    per_unit = len(grad_copies) // units
    ahead = min(AHEAD, acts)
    for copy in grad_copies[:per_unit] + value_copies[: 2 * ahead] + grad_copies[per_unit:] + extra_copies:
        copy.start()
    waited = 0
    done = 0
    for u in range(units):
        for copy in grad_copies[u * per_unit : (u + 1) * per_unit]:
            copy.wait()
        for first, count, out_first, extra_first in jobs[u]:
            if extra_first is not None:
                for copy in extra_copies:
                    copy.wait()
                extra_copies = []

            def step(j, carry, u=u, first=first, out_first=out_first, waited=waited, extra_first=extra_first):
                @pl.when(first + j >= waited)
                def _():
                    for seq in range(2):
                        pltpu.make_async_copy(
                            act_refs[0][seq].at[:, :, pl.ds(0, QUARTER)],
                            values.at[first + j, seq],
                            value_sem.at[first + j, seq],
                        ).wait()
                    for a in range(max(ahead, first + ahead), min(acts, first + count + ahead)):

                        @pl.when(first + j + ahead == a)
                        def _(a=a):
                            value_copies[2 * a].start()
                            value_copies[2 * a + 1].start()

                act = values[first + j].reshape(-1, QUARTER)
                tile = jnp.dot(grads[u], act, preferred_element_type=jnp.float32)
                at = out_first + j
                if extra_first is not None:
                    start = pl.multiple_of((extra_first + j) * QUARTER, QUARTER)
                    tile = tile + added[0][:, pl.ds(start, QUARTER)].astype(jnp.float32)
                results[at] = tile.astype(results.dtype)
                for part in range(NZ):
                    pltpu.make_async_copy(
                        results.at[at, pl.ds(part * ROWS, ROWS), :],
                        outs[part].at[:, pl.ds(pl.multiple_of(at * QUARTER, QUARTER), QUARTER)],
                        result_sem.at[at, part],
                    ).start()
                return carry

            lax.fori_loop(0, count, step, 0)
            waited = max(waited, first + count)
            done += count

    def settle(at, carry):
        for part in range(NZ):
            pltpu.make_async_copy(
                results.at[at, pl.ds(part * ROWS, ROWS), :],
                outs[part].at[:, pl.ds(pl.multiple_of(at * QUARTER, QUARTER), QUARTER)],
                result_sem.at[at, part],
            ).wait()
        return carry

    lax.fori_loop(0, done, settle, 0)


def products(pieces, acts, jobs, extra=(), whole=False):
    units, count = len(pieces), 2 * len(acts)
    total = sum(n for runs in jobs for _, n, *_ in runs)
    operands = [a for piece in pieces for a in piece] + [a for pair in acts for a in pair] + list(extra)
    tokens = pieces[0][0].shape[-1]
    shape = acts[0][0].shape[:2] + (QUARTER,)
    shapes = (NZ * ROWS,) if whole else (ROWS,) * NZ
    flops = 2 * total * QUARTER * NZ * ROWS * 2 * shape[0] * shape[1]
    return pl.pallas_call(
        functools.partial(product_kernel, jobs=jobs, units=units, acts=count, extra=len(extra), whole=whole),
        in_specs=[pl.BlockSpec(memory_space=pl.ANY)] * len(operands),
        out_specs=[pl.BlockSpec(memory_space=pl.ANY)] * len(shapes),
        out_shape=[jax.ShapeDtypeStruct((rows, total * QUARTER), jnp.bfloat16) for rows in shapes],
        scratch_shapes=[
            pltpu.VMEM((units, NZ * ROWS, 4 * NX * tokens), jnp.bfloat16),
            pltpu.VMEM((count, 2) + shape, jnp.bfloat16),
            pltpu.VMEM((total, NZ * ROWS, QUARTER), jnp.bfloat16),
            pltpu.SemaphoreType.DMA((units, 4 * NX)),
            pltpu.SemaphoreType.DMA((count, 2)),
            pltpu.SemaphoreType.DMA((total, NZ)),
        ]
        + ([pltpu.VMEM((NZ * ROWS, extra[0].shape[1]), jnp.bfloat16), pltpu.SemaphoreType.DMA((1,))] if extra else []),
        cost_estimate=pl.CostEstimate(flops=flops, bytes_accessed=2**20, transcendentals=0),
    )(*operands)


def reduce_over_z(parts, upward, hold):
    f32 = jnp.float32
    far, up, down, own = parts
    late, soon = (up, down) if upward else (down, up)
    onward, back = (Z_UP, Z_DOWN) if upward else (Z_DOWN, Z_UP)
    passing = send(far, onward)
    if hold is not None:
        passing, _ = lax.optimization_barrier((passing, hold))
    joined = (late.astype(f32) + passing.astype(f32)).astype(late.dtype)
    soon_sum = send(soon, back)
    late_sum = send(joined, onward)
    return own, soon_sum, late_sum, joined


HEADS_PER_HALF = 2 * QUARTER // HEAD_DIM

PORTIONS = (
    ("pa", None, ((0, "own", 0, 4),)),
    ("pb", True, ((0, "y", 0, 2), (1, "own", 0, 4))),
    ("pc", False, ((0, "y", 2, 2), (1, "y", 2, 2), (1, "y", 0, 2))),
    ("pd", False, ((2, "own", 0, 4), (2, "y", 0, 4))),
    ("pe", True, ((3, "own", 0, 4), (3, "y", 0, 4))),
)
OUTER = (("pb", "pc"), ("pd",))


def program(saved_queries, saved_keys, saved_values, out_grad, act_exponent, grad_exponent):
    f32, bf16 = jnp.float32, jnp.bfloat16
    yh, _, c, yl, _ = position()
    chip = yl ^ yh
    dequant = jnp.exp2((act_exponent[0] + grad_exponent[0]).astype(f32)) / (SATURATION * SATURATION)

    blocks = quantize_columns(grad_exponent, out_grad, FIRST)
    blocks |= quantize_columns(grad_exponent, out_grad, REST)
    near_sent = [send(blocks[1, 0, *group], CORES) for group in ((0, 1), (1, 3))]
    theirs = [near_sent[0][0], *(near_sent[1][i] for i in range(3))]
    mine = [blocks[0, 0, unit, 1][0] for unit in range(UNITS)]

    acts = {}
    for half in range(2):
        a = attend(act_exponent, saved_queries, saved_keys, saved_values, half * HEADS_PER_HALF, HEADS_PER_HALF)
        acts["own", half] = (a, send(a, CORES))
        b = send(a, Y_INNER)
        acts["y", half] = (b, send(b, CORES))

    from_y = {}
    for first, count in GROUPS:
        near = send(blocks[0, 1, first, count], Y_INNER)
        other = send(send(blocks[1, 1, first, count], CORES), Y_INNER)
        if count > 1:
            near, other, _ = lax.optimization_barrier((near, other, acts["own", 1][0]))
        for unit in range(first, first + count):
            from_y[unit] = (near[unit - first], other[unit - first])

    pieces = []
    for unit in range(UNITS):
        block = jnp.stack([mine[unit], from_y[unit][0], theirs[unit], from_y[unit][1]])
        block = block.reshape((2, 2) + block.shape[1:])
        left = send(block, X_UP)
        right = send(block, X_DOWN)
        far = send(left, X_UP) if unit % 2 == 0 else send(right, X_DOWN)
        pieces.append((block, left, right, far))

    made = {}
    direct = ()
    for name, upward, runs in PORTIONS:
        units, used, jobs, at = [], [], [], 0
        for unit, side, first, count in runs:
            if unit not in units:
                units.append(unit)
                jobs.append([])
            for quarter in range(first, first + count):
                if (side, quarter) not in used:
                    used.append((side, quarter))
            joins = first if (unit, side) == (1, "y") else None
            jobs[units.index(unit)].append((used.index((side, first)), count, at, joins))
            at += count
        halves = [acts[side, quarter // 2] for side, quarter in used[::2]]
        extra = direct if any(run[3] is not None for runs_of in jobs for run in runs_of) else ()
        made[name] = products([pieces[u] for u in units], halves, jobs, extra, upward is None)
        if upward is None:
            direct = (send(made[name][0], Y_OUTER),)

    sums = {}
    leaving = {}
    joined = {}
    for index, (name, upward, runs) in enumerate(PORTIONS):
        if upward is None:
            continue
        later = made[PORTIONS[index + 1][0]][3] if index + 1 < len(PORTIONS) else None
        own, below, above, joined[name] = reduce_over_z(made[name], upward, later)
        at = 0
        leaving[name] = []
        for unit, side, first, count in runs:
            for k in range(count):
                sums[unit, side, first + k] = (own, below, above, at)
                if unit % 2 == 0:
                    leaving[name].append((unit, side, first + k))
                at += 1

    outgoing, out_places = {}, []
    for index, names in enumerate(OUTER):
        at, columns = 0, []
        for name in names:
            cut = len(leaving[name]) * QUARTER
            own, below, above, _ = sums[leaving[name][0]]
            if index == 0:
                own, below, above, _ = lax.optimization_barrier((own, below, above, joined["pd"]))
            columns.append(own[:, :cut].astype(f32) + below[:, :cut].astype(f32) + above[:, :cut].astype(f32))
            for key in leaving[name]:
                out_places.append((*key, index, at))
                at += 1
        message = jnp.concatenate(columns, 1).astype(bf16)
        outgoing[index] = send(message, Y_OUTER)
        outgoing[index], _ = lax.optimization_barrier((outgoing[index], joined["pe"]))

    incoming = {}
    for unit, side, quarter, name, at in out_places:
        incoming[unit + 1, "y" if side == "own" else "own", quarter] = (outgoing[name], at)

    def total(unit, side, hold=None):
        columns = []
        for quarter in range(4):
            own, below, above, at = sums[unit, side, quarter]
            parts = [(own, at), (below, at), (above, at)]
            if (unit, side, quarter) in incoming:
                parts.append(incoming[unit, side, quarter])
            if hold is not None:
                arrays = lax.optimization_barrier((*(a for a, _ in parts), hold))
                parts = [(a, where) for a, (_, where) in zip(arrays[:-1], parts, strict=True)]
            columns.append(sum(a[:, w * QUARTER : (w + 1) * QUARTER].astype(f32) for a, w in parts))
        return jnp.concatenate(columns, 1)

    keeps, gifts = [], []
    for half in range(2):
        unit = 2 * half + 1
        leaves = total(unit, "y").astype(bf16)
        swapped = send(leaves, Y_INNER)
        near = total(unit, "own", leaves)
        stays = chip == c
        keeps.append(jnp.where(stays, near, swapped.astype(f32)))
        gifts.append(send(jnp.where(stays, swapped, near.astype(bf16)), CORES).astype(f32))
    keep, gift = jnp.concatenate(keeps, 0), jnp.concatenate(gifts, 0)
    result = jnp.where(c == 0, jnp.stack([keep, gift]), jnp.stack([gift, keep])) * dequant
    return result.reshape(4 * ROWS, -1)


def solution(mesh):
    in_specs = (
        P("dp", "tensor"),
        P("dp", "tensor"),
        P("dp", "tensor"),
        P(("dp", "tensor"), None),
        P(),
        P(),
    )
    out_specs = P("dp", "tensor")
    return jax.shard_map(program, mesh=mesh, in_specs=in_specs, out_specs=out_specs, check_vma=False)
```

```python
import functools

import jax
import jax.numpy as jnp
from jax import lax
from jax.experimental import pallas as pl
from jax.experimental.pallas import tpu as pltpu
from jax.sharding import PartitionSpec as P


HEAD_DIM = 128
SATURATION = 448.0
NY, NZ, NC, NX = 2, 4, 2, 4
AXES = ("dp", "tensor")
UNITS = 4
ROWS = 128
STEPS = (2, 1, 3, 0)
QUARTER = 256
AHEAD = 2


def device_of(yh, z, c, yl, x):
    return ((yh * NZ + z) * NC + c) * (NY * NX) + yl * NX + x


def pairs_of(target):
    pairs = []
    for yh in range(NY):
        for z in range(NZ):
            for c in range(NC):
                for yl in range(NY):
                    for x in range(NX):
                        pairs.append((device_of(yh, z, c, yl, x), device_of(*target(yh, z, c, yl, x))))
    return pairs


X_UP = pairs_of(lambda yh, z, c, yl, x: (yh, z, c, yl, (x + 1) % NX))
X_DOWN = pairs_of(lambda yh, z, c, yl, x: (yh, z, c, yl, (x - 1) % NX))
Z_UP = pairs_of(lambda yh, z, c, yl, x: (yh, (z + 1) % NZ, c, yl, x))
Z_DOWN = pairs_of(lambda yh, z, c, yl, x: (yh, (z - 1) % NZ, c, yl, x))
Y_INNER = pairs_of(lambda yh, z, c, yl, x: (yh, z, c, 1 - yl, x))
Y_OUTER = pairs_of(lambda yh, z, c, yl, x: (1 - yh, z, c, 1 - yl, x))
CORES = pairs_of(lambda yh, z, c, yl, x: (yh, z, 1 - c, yl, x))


def send(block, pairs):
    return lax.ppermute(block, AXES, pairs)


def position():
    place = lax.axis_index("dp")
    side = lax.axis_index("tensor")
    return place // (NZ * NC), place // NC % NZ, place % NC, side // NX, side % NX


def saturation_factor(exponent_ref, width):
    exponent = jnp.full((1, width), -exponent_ref[0].astype(jnp.float32))
    return SATURATION * jnp.exp2(exponent)


GROUPS = ((0, 1), (1, 1), (2, 2))
FIRST = ((1, 1, 0, 1), (0, 1, 0, 1), (1, 0, 0, 1), (0, 0, 0, 1))
REST = ((1, 0, 1, 3), (1, 1, 1, 1), (1, 1, 2, 2)) + tuple((0, 0, u, 1) for u in (1, 2, 3)) + ((0, 1, 1, 1), (0, 1, 2, 2))


def quantize_kernel(exponent_ref, grad_ref, *out_refs, made):
    yh, z, c, yl, _ = position()
    factor = saturation_factor(exponent_ref, ROWS)
    for (other_core, far_chip, first, count), ref in zip(made, out_refs, strict=True):
        chip = (yl ^ yh) ^ far_chip
        core = c ^ other_core
        for unit in range(first, first + count):
            for step in range(NZ):
                yh_at = yh if unit % 2 else 1 - yh
                z_at = lax.rem(z + STEPS[step], NZ)
                column = 4 * (8 * yh_at + 2 * z_at + chip) + 2 * core + unit // 2
                values = grad_ref[:, pl.ds(pl.multiple_of(column * ROWS, ROWS), ROWS)].astype(jnp.float32)
                scaled = jnp.clip(values * factor, -SATURATION, SATURATION).astype(jnp.bfloat16)
                ref[unit - first, step * ROWS : (step + 1) * ROWS, :] = scaled.T


def quantize_columns(exponent, out_grad, made):
    tokens = out_grad.shape[0]
    arrays = pl.pallas_call(
        functools.partial(quantize_kernel, made=made),
        in_specs=[pl.BlockSpec(memory_space=pltpu.SMEM), pl.BlockSpec(memory_space=pltpu.VMEM)],
        out_specs=[pl.BlockSpec(memory_space=pltpu.VMEM)] * len(made),
        out_shape=[jax.ShapeDtypeStruct((n, NZ * ROWS, tokens), jnp.bfloat16) for *_, n in made],
        cost_estimate=pl.CostEstimate(flops=2 * 10**9, bytes_accessed=3 * 2**20, transcendentals=0),
    )(exponent, out_grad)
    return dict(zip(made, arrays, strict=True))


Q_BLOCK = 256
LOG2_E = 1.4426950408889634


def attention_kernel(exponent_ref, query_ref, key_ref, value_ref, out_ref):
    _, _, _, _, x = position()
    seq_len = key_ref.shape[0]
    scale = HEAD_DIM**-0.5 * LOG2_E
    factor = saturation_factor(exponent_ref, HEAD_DIM)
    row = lax.broadcasted_iota(jnp.int32, (Q_BLOCK, Q_BLOCK), 0)
    column = lax.broadcasted_iota(jnp.int32, (Q_BLOCK, Q_BLOCK), 1)
    causal = column <= row

    def scores_of(start):
        queries = query_ref[start : start + Q_BLOCK, :]

        def block(first, last):
            return lax.dot_general(
                queries, key_ref[first:last, :], (((1,), (1,)), ((), ())), preferred_element_type=jnp.float32
            )

        return block(start, start + Q_BLOCK), block(0, start) if start else None

    def weights_of(near, past):
        near = jnp.where(causal, near, jnp.float32(-1e30))
        row_max = jnp.max(near, axis=1, keepdims=True)
        if past is not None:
            row_max = jnp.maximum(row_max, jnp.max(past, axis=1, keepdims=True))
        near = jnp.exp2((near - row_max) * scale)
        total = jnp.sum(near, axis=1, keepdims=True)
        if past is not None:
            past = jnp.exp2((past - row_max) * scale)
            total = total + jnp.sum(past, axis=1, keepdims=True)
            past = past.astype(jnp.bfloat16)
        return near.astype(jnp.bfloat16), past, total

    def finish(start, near, past, total):
        mixed = jnp.dot(near, value_ref[start : start + Q_BLOCK, :], preferred_element_type=jnp.float32)
        if past is not None:
            mixed = mixed + jnp.dot(past, value_ref[:start, :], preferred_element_type=jnp.float32)
        scaled = jnp.clip(mixed / total * factor, -SATURATION, SATURATION).astype(jnp.bfloat16)
        for part in range(Q_BLOCK // ROWS):
            token_block = start // ROWS + part
            ahead = lax.rem(token_block % NX - x + NX, NX)
            order = jnp.where(ahead == 0, 0, jnp.where(ahead == 3, 1, ahead + 1))
            out_ref[pl.ds(order * 2 + token_block // NX, 1)] = scaled[part * ROWS : (part + 1) * ROWS][None]

    scores, waiting = scores_of(0), None
    for start in range(0, seq_len, Q_BLOCK):
        following = scores_of(start + Q_BLOCK) if start + Q_BLOCK < seq_len else None
        weights = weights_of(*scores)
        if waiting is not None:
            finish(*waiting)
        waiting, scores = (start, *weights), following
    finish(*waiting)


def attend(exponent, queries, keys, values, first, heads):
    seq_len = queries.shape[0]
    blocks = seq_len // ROWS
    return pl.pallas_call(
        attention_kernel,
        grid=(heads,),
        in_specs=[
            pl.BlockSpec(memory_space=pltpu.SMEM),
            pl.BlockSpec((seq_len, HEAD_DIM), lambda h: (0, h + first)),
            pl.BlockSpec((seq_len, HEAD_DIM), lambda h: (0, 0)),
            pl.BlockSpec((seq_len, HEAD_DIM), lambda h: (0, 0)),
        ],
        out_specs=pl.BlockSpec((blocks, ROWS, HEAD_DIM), lambda h: (0, 0, h)),
        out_shape=jax.ShapeDtypeStruct((blocks, ROWS, heads * HEAD_DIM), jnp.bfloat16),
        cost_estimate=pl.CostEstimate(flops=4 * 10**9, bytes_accessed=2**20, transcendentals=0),
    )(exponent, queries, keys, values)


def product_kernel(*refs, jobs, units, acts, extra, whole):
    piece_refs = [refs[4 * u : 4 * u + 4] for u in range(units)]
    act_refs = [refs[4 * units + 2 * a : 4 * units + 2 * a + 2] for a in range(acts // 2)]
    refs = refs[4 * units + acts :]
    extra_refs, refs = refs[:extra], refs[extra:]
    if whole:
        outs = [refs[0].at[pl.ds(part * ROWS, ROWS), :] for part in range(NZ)]
    else:
        outs = refs[:NZ]
    grads, values, results, grad_sem, value_sem, result_sem, *added = refs[1 if whole else NZ :]
    extra_copies = [pltpu.make_async_copy(ref, added[0], added[1].at[0]) for ref in extra_refs]
    yl = position()[3]
    grad_copies = []
    for u in range(units):
        for seq in range(2):
            for source in range(NX):
                for row in range(2):
                    at = (seq * NX + source) * 2 + row
                    grad_copies.append(
                        pltpu.make_async_copy(
                            piece_refs[u][source].at[seq, row ^ yl],
                            grads.at[u, :, pl.ds(at * ROWS, ROWS)],
                            grad_sem.at[u, at],
                        )
                    )
    value_copies = [
        pltpu.make_async_copy(
            act_refs[a // 2][seq].at[:, :, pl.ds(a % 2 * QUARTER, QUARTER)], values.at[a, seq], value_sem.at[a, seq]
        )
        for a in range(acts)
        for seq in range(2)
    ]
    per_unit = len(grad_copies) // units
    ahead = min(AHEAD, acts)
    for copy in grad_copies[:per_unit] + value_copies[: 2 * ahead] + grad_copies[per_unit:] + extra_copies:
        copy.start()
    waited = 0
    done = 0
    for u in range(units):
        for copy in grad_copies[u * per_unit : (u + 1) * per_unit]:
            copy.wait()
        for first, count, out_first, extra_first in jobs[u]:
            if extra_first is not None:
                for copy in extra_copies:
                    copy.wait()
                extra_copies = []

            def step(j, carry, u=u, first=first, out_first=out_first, waited=waited, extra_first=extra_first):
                @pl.when(first + j >= waited)
                def _():
                    for seq in range(2):
                        pltpu.make_async_copy(
                            act_refs[0][seq].at[:, :, pl.ds(0, QUARTER)],
                            values.at[first + j, seq],
                            value_sem.at[first + j, seq],
                        ).wait()
                    for a in range(max(ahead, first + ahead), min(acts, first + count + ahead)):

                        @pl.when(first + j + ahead == a)
                        def _(a=a):
                            value_copies[2 * a].start()
                            value_copies[2 * a + 1].start()

                act = values[first + j].reshape(-1, QUARTER)
                tile = jnp.dot(grads[u], act, preferred_element_type=jnp.float32)
                at = out_first + j
                if extra_first is not None:
                    start = pl.multiple_of((extra_first + j) * QUARTER, QUARTER)
                    tile = tile + added[0][:, pl.ds(start, QUARTER)].astype(jnp.float32)
                results[at] = tile.astype(results.dtype)
                for part in range(NZ):
                    pltpu.make_async_copy(
                        results.at[at, pl.ds(part * ROWS, ROWS), :],
                        outs[part].at[:, pl.ds(pl.multiple_of(at * QUARTER, QUARTER), QUARTER)],
                        result_sem.at[at, part],
                    ).start()
                return carry

            lax.fori_loop(0, count, step, 0)
            waited = max(waited, first + count)
            done += count

    def settle(at, carry):
        for part in range(NZ):
            pltpu.make_async_copy(
                results.at[at, pl.ds(part * ROWS, ROWS), :],
                outs[part].at[:, pl.ds(pl.multiple_of(at * QUARTER, QUARTER), QUARTER)],
                result_sem.at[at, part],
            ).wait()
        return carry

    lax.fori_loop(0, done, settle, 0)


def products(pieces, acts, jobs, extra=(), whole=False):
    units, count = len(pieces), 2 * len(acts)
    total = sum(n for runs in jobs for _, n, *_ in runs)
    operands = [a for piece in pieces for a in piece] + [a for pair in acts for a in pair] + list(extra)
    tokens = pieces[0][0].shape[-1]
    shape = acts[0][0].shape[:2] + (QUARTER,)
    shapes = (NZ * ROWS,) if whole else (ROWS,) * NZ
    flops = 2 * total * QUARTER * NZ * ROWS * 2 * shape[0] * shape[1]
    return pl.pallas_call(
        functools.partial(product_kernel, jobs=jobs, units=units, acts=count, extra=len(extra), whole=whole),
        in_specs=[pl.BlockSpec(memory_space=pl.ANY)] * len(operands),
        out_specs=[pl.BlockSpec(memory_space=pl.ANY)] * len(shapes),
        out_shape=[jax.ShapeDtypeStruct((rows, total * QUARTER), jnp.bfloat16) for rows in shapes],
        scratch_shapes=[
            pltpu.VMEM((units, NZ * ROWS, 4 * NX * tokens), jnp.bfloat16),
            pltpu.VMEM((count, 2) + shape, jnp.bfloat16),
            pltpu.VMEM((total, NZ * ROWS, QUARTER), jnp.bfloat16),
            pltpu.SemaphoreType.DMA((units, 4 * NX)),
            pltpu.SemaphoreType.DMA((count, 2)),
            pltpu.SemaphoreType.DMA((total, NZ)),
        ]
        + ([pltpu.VMEM((NZ * ROWS, extra[0].shape[1]), jnp.bfloat16), pltpu.SemaphoreType.DMA((1,))] if extra else []),
        cost_estimate=pl.CostEstimate(flops=flops, bytes_accessed=2**20, transcendentals=0),
    )(*operands)


def reduce_over_z(parts, upward, hold, pieces=1):
    f32 = jnp.float32
    far, up, down, own = parts
    late, soon = (up, down) if upward else (down, up)
    onward, back = (Z_UP, Z_DOWN) if upward else (Z_DOWN, Z_UP)
    passing = send(far, onward)
    if hold is not None:
        passing, _ = lax.optimization_barrier((passing, hold))
    soon_sum = send(soon, back)
    width = late.shape[1] // pieces
    joined, late_sums = [], []
    for piece in range(pieces):
        cut = slice(piece * width, (piece + 1) * width)
        joined.append((late[:, cut].astype(f32) + passing[:, cut].astype(f32)).astype(late.dtype))
        late_sums.append(send(joined[-1], onward))
    return own, soon_sum, late_sums, joined[0]


HEADS_PER_HALF = 2 * QUARTER // HEAD_DIM

PORTIONS = (
    ("pa", None, ((0, "own", 0, 4),)),
    ("pb", True, ((0, "y", 0, 2), (1, "own", 0, 4))),
    ("pc", False, ((0, "y", 2, 2), (1, "y", 2, 2), (1, "y", 0, 2))),
    ("pd", False, ((2, "own", 0, 4), (2, "y", 0, 4))),
    ("pe", True, ((3, "own", 0, 4), (3, "y", 0, 4))),
)
OUTER = (("pb", "pc"), ("pd",))


def program(saved_queries, saved_keys, saved_values, out_grad, act_exponent, grad_exponent):
    f32, bf16 = jnp.float32, jnp.bfloat16
    yh, _, c, yl, _ = position()
    chip = yl ^ yh
    dequant = jnp.exp2((act_exponent[0] + grad_exponent[0]).astype(f32)) / (SATURATION * SATURATION)

    blocks = quantize_columns(grad_exponent, out_grad, FIRST)
    blocks |= quantize_columns(grad_exponent, out_grad, REST)
    near_sent = [send(blocks[1, 0, *group], CORES) for group in ((0, 1), (1, 3))]
    theirs = [near_sent[0][0], *(near_sent[1][i] for i in range(3))]
    mine = [blocks[0, 0, unit, 1][0] for unit in range(UNITS)]

    acts = {}
    for half in range(2):
        a = attend(act_exponent, saved_queries, saved_keys, saved_values, half * HEADS_PER_HALF, HEADS_PER_HALF)
        acts["own", half] = (a, send(a, CORES))
        b = send(a, Y_INNER)
        acts["y", half] = (b, send(b, CORES))

    from_y = {}
    for first, count in GROUPS:
        near = send(blocks[0, 1, first, count], Y_INNER)
        other = send(send(blocks[1, 1, first, count], CORES), Y_INNER)
        if count > 1:
            near, other, _ = lax.optimization_barrier((near, other, acts["own", 1][0]))
        for unit in range(first, first + count):
            from_y[unit] = (near[unit - first], other[unit - first])

    pieces = []
    for unit in range(UNITS):
        block = jnp.stack([mine[unit], from_y[unit][0], theirs[unit], from_y[unit][1]])
        block = block.reshape((2, 2) + block.shape[1:])
        left = send(block, X_UP)
        right = send(block, X_DOWN)
        far = send(left, X_UP) if unit % 2 == 0 else send(right, X_DOWN)
        pieces.append((block, left, right, far))

    made = {}
    direct = ()
    for name, upward, runs in PORTIONS:
        units, used, jobs, at = [], [], [], 0
        for unit, side, first, count in runs:
            if unit not in units:
                units.append(unit)
                jobs.append([])
            for quarter in range(first, first + count):
                if (side, quarter) not in used:
                    used.append((side, quarter))
            joins = first if (unit, side) == (1, "y") else None
            jobs[units.index(unit)].append((used.index((side, first)), count, at, joins))
            at += count
        halves = [acts[side, quarter // 2] for side, quarter in used[::2]]
        extra = direct if any(run[3] is not None for runs_of in jobs for run in runs_of) else ()
        made[name] = products([pieces[u] for u in units], halves, jobs, extra, upward is None)
        if upward is None:
            direct = (send(made[name][0], Y_OUTER),)

    def following_exists(index):
        return index + 1 < len(PORTIONS)

    sums = {}
    leaving = {}
    joined = {}
    for index, (name, upward, runs) in enumerate(PORTIONS):
        if upward is None:
            continue
        later = made[PORTIONS[index + 1][0]][3] if index + 1 < len(PORTIONS) else None
        pieces_of = 1 if following_exists(index) else 2
        own, soon, late, joined[name] = reduce_over_z(made[name], upward, later, pieces_of)
        at = 0
        leaving[name] = []
        for unit, side, first, count in runs:
            for k in range(count):
                piece, late_at = (0, at) if len(late) == 1 else divmod(at, 4)
                sums[unit, side, first + k] = (own, soon, late[piece], at, late_at)
                if unit % 2 == 0:
                    leaving[name].append((unit, side, first + k))
                at += 1

    outgoing, out_places = {}, []
    for index, names in enumerate(OUTER):
        at, columns = 0, []
        for name in names:
            cut = len(leaving[name]) * QUARTER
            own, below, above, *_ = sums[leaving[name][0]]
            if index == 0:
                own, below, above, _ = lax.optimization_barrier((own, below, above, joined["pd"]))
            columns.append(own[:, :cut].astype(f32) + below[:, :cut].astype(f32) + above[:, :cut].astype(f32))
            for key in leaving[name]:
                out_places.append((*key, (index, at // 4), at % 4))
                at += 1
        whole = jnp.concatenate(columns, 1)
        for piece in range(at // 4):
            message = whole[:, piece * 4 * QUARTER : (piece + 1) * 4 * QUARTER].astype(bf16)
            arrived = send(message, Y_OUTER)
            outgoing[index, piece], _ = lax.optimization_barrier((arrived, joined["pe"]))

    incoming = {}
    for unit, side, quarter, name, at in out_places:
        incoming[unit + 1, "y" if side == "own" else "own", quarter] = (outgoing[name], at)

    def total(unit, side, hold=None):
        columns = []
        for quarter in range(4):
            own, below, above, at, late_at = sums[unit, side, quarter]
            parts = [(own, at), (below, at), (above, late_at)]
            if (unit, side, quarter) in incoming:
                parts.append(incoming[unit, side, quarter])
            if hold is not None:
                arrays = lax.optimization_barrier((*(a for a, _ in parts), hold))
                parts = [(a, where) for a, (_, where) in zip(arrays[:-1], parts, strict=True)]
            columns.append(sum(a[:, w * QUARTER : (w + 1) * QUARTER].astype(f32) for a, w in parts))
        return jnp.concatenate(columns, 1)

    keeps, gifts = [], []
    for half in range(2):
        unit = 2 * half + 1
        leaves = total(unit, "y").astype(bf16)
        swapped = send(leaves, Y_INNER)
        near = total(unit, "own", leaves)
        stays = chip == c
        keeps.append(jnp.where(stays, near, swapped.astype(f32)))
        gifts.append(send(jnp.where(stays, swapped, near.astype(bf16)), CORES).astype(f32))
    keep, gift = jnp.concatenate(keeps, 0), jnp.concatenate(gifts, 0)
    result = jnp.where(c == 0, jnp.stack([keep, gift]), jnp.stack([gift, keep])) * dequant
    return result.reshape(4 * ROWS, -1)


def solution(mesh):
    in_specs = (
        P("dp", "tensor"),
        P("dp", "tensor"),
        P("dp", "tensor"),
        P(("dp", "tensor"), None),
        P(),
        P(),
    )
    out_specs = P("dp", "tensor")
    return jax.shard_map(program, mesh=mesh, in_specs=in_specs, out_specs=out_specs, check_vma=False)
```
